256 devices in a mesh: groups: 2 (over z), blk: 64 (over y, x), rep: 2 (over core).
Axes of the slice: x: 8, y: 8, z: 2, core: 2. Of those that a mesh axis runs over, the one named last changes fastest.
The devices are a block of a 8x8x16 slice.
Arguments:
- tokens: bfloat16 [16384, 7168], P(('groups', 'blk', 'rep')), parts along dimension 0, may hold values from -6 to 6
- router_scores: float32 [16384, 8], P(('groups', 'blk', 'rep')), parts along dimension 0, may hold values from -6 to 6
- expert_ids: int32 [16384, 8], P(('groups', 'blk', 'rep')), parts along dimension 0, may hold values from 0 to 255, as said below
- gate_weight: bfloat16 [7168, 32768], P(None, ('blk', 'rep')), may hold values from -0.0625 to 0.0625
- up_weight: bfloat16 [7168, 32768], P(None, ('blk', 'rep')), may hold values from -0.0625 to 0.0625
- down_weight: bfloat16 [32768, 7168], P(('blk', 'rep')), may hold values from -0.125 to 0.125
Outputs:
- moe_out: bfloat16 [16384, 7168], P(('groups', 'blk', 'rep')), parts along dimension 0
The draws below stay inside these ranges and needn't reach their ends.
There are 2 independent parts, one for each index of `groups`. The reference program is written for one: setup_inputs(seed, part) draws one part's arguments, and reference() takes and returns one part's arrays. A program takes and returns all parts, laid end to end along the dimension named above; an argument that names none is the same for every part. Nothing has to cross between parts.
Inputs may be any that keep to these rules, and one draw needn't show every extreme that they name: `expert_ids`: each row names 8 different experts. In the rows of one device (aligned blocks of 64 rows) each expert below 16 is named by at most 2 rows, and in every draw one such expert is named by exactly 2 rows in every block.
All inputs are finite; a program needn't handle non-finite values.
Results may differ from the reference program's by a relative error of at most 0.0068.
Values may be sent and summed in bfloat16 or wider, within the bound.
A program may use at most 128 MiB of HBM per device.

```python
import jax
import jax.numpy as jnp
from jax import lax

D = 7168
FF = 2048
EXPERTS = 256
TOP = 8
TOK_DEV = 64
CAP = 2
EXP_WIN = 16
TOKENS = 8192


def draw_block(block_key, hot_expert, expert_caps):
    key_count, key_rows, key_offset, key_order = jax.random.split(block_key, 4)
    counts = jax.random.randint(key_count, (EXP_WIN,), 0, expert_caps + 1)
    counts = jnp.where(jnp.arange(EXP_WIN) == hot_expert, CAP, counts)
    item_ends = jnp.cumsum(counts)
    total_items = item_ends[-1]
    item_index = jnp.arange(EXP_WIN * CAP)
    owners = jnp.sum((item_ends[None, :] <= item_index[:, None]).astype(jnp.int32), axis=1)
    is_valid = item_index < total_items
    row_order = jax.random.permutation(key_rows, TOK_DEV)
    item_row = jnp.where(is_valid, row_order[item_index % TOK_DEV], TOK_DEV)
    item_slot = item_index // TOK_DEV
    offsets = jax.random.randint(key_offset, (TOK_DEV, 1), 0, EXPERTS - EXP_WIN)
    outer_ids = EXP_WIN + (offsets + jnp.arange(TOP)[None, :]) % (EXPERTS - EXP_WIN)
    id_table = outer_ids.at[item_row, item_slot].set(owners, mode='drop')
    order_keys = jax.random.split(key_order, TOK_DEV)
    orders = jax.vmap(lambda one_key: jax.random.permutation(one_key, TOP))(order_keys)
    return jnp.take_along_axis(id_table, orders, axis=1).astype(jnp.int32)


def draw_expert_ids(key, part):
    num_blocks = TOKENS // TOK_DEV
    key_hot, key_caps, key_rest = jax.random.split(key, 3)
    hot_expert = jax.random.randint(key_hot, (), 0, EXP_WIN)
    expert_caps = jax.random.randint(key_caps, (EXP_WIN,), CAP // 2, CAP + 1)
    block_keys = jax.random.split(key_rest, num_blocks)
    id_blocks = jax.vmap(lambda one_key: draw_block(one_key, hot_expert, expert_caps))(block_keys)
    return id_blocks.reshape(TOKENS, TOP).astype(jnp.int32)


def steps_of(own_key, shape, cuts, low, high):
    def one(axis_at, shards_of):
        heights = jax.random.uniform(jax.random.fold_in(jax.random.fold_in(own_key, 6), axis_at), (shards_of,), jnp.float32, low / len(cuts), high / len(cuts))
        return jnp.repeat(jnp.exp(heights), shape[axis_at] // shards_of).reshape((-1,) + (1,) * (len(shape) - axis_at - 1))

    loudness = one(*cuts[0])
    for cut in cuts[1:]:
        loudness = loudness * one(*cut)
    return loudness


def noise(rng, dims, spread, most, pieces=(), kind=jnp.bfloat16):
    values = spread * jax.random.normal(rng, dims, jnp.float32)
    if pieces:
        values = values * steps_of(rng, dims, pieces, -0.22, 0.18)
    return jnp.clip(values, -most, most).astype(kind)


def setup_inputs(seed: int = 0, part: int = 0) -> dict:
    key_of = jax.random.split(jax.random.key(seed), 7)
    part_splits = jax.random.split(jax.random.fold_in(key_of[6], part), 7)
    return {
        "tokens": noise(part_splits[0], (TOKENS, D), 1.0, 6.0, ((0, 128),)),
        "router_scores": noise(part_splits[1], (TOKENS, TOP), 1.5, 6.0, ((0, 128),), jnp.float32),
        "expert_ids": draw_expert_ids(jax.random.fold_in(jax.random.fold_in(key_of[6], part), 71), part),
        "gate_weight": noise(key_of[3], (D, EXP_WIN * FF), D ** -0.5, 0.0625, ((1, 128),)),
        "up_weight": noise(key_of[4], (D, EXP_WIN * FF), D ** -0.5, 0.0625, ((1, 128),)),
        "down_weight": noise(key_of[5], (EXP_WIN * FF, D), FF ** -0.5, 0.125, ((0, 128),)),
    }


route_scale = 2.5


def reference(tokens, router_scores, expert_ids, gate_weight, up_weight, down_weight):
    sigmoid_scores = jax.nn.sigmoid(router_scores.astype(jnp.float32))
    gate_values = route_scale * sigmoid_scores / jnp.sum(sigmoid_scores, axis=1, keepdims=True)
    row_limit = CAP * (TOKENS // TOK_DEV)

    def one_expert(running, expert):
        member = expert_ids == expert
        weight_row = jnp.sum(jnp.where(member, gate_values, jnp.float32(0.0)), axis=1)
        is_named = jnp.any(member, axis=1)
        named_count = jnp.sum(is_named.astype(jnp.int32))
        positions = jnp.nonzero(is_named, size=row_limit, fill_value=0)[0].astype(jnp.int32)
        is_valid = jnp.arange(row_limit, dtype=jnp.int32) < named_count
        picked_rows = tokens[positions]
        first_unit = (expert * FF).astype(jnp.int32)
        w_gate = lax.dynamic_slice_in_dim(gate_weight, first_unit, FF, 1)
        w_up = lax.dynamic_slice_in_dim(up_weight, first_unit, FF, 1)
        w_down = lax.dynamic_slice_in_dim(down_weight, first_unit, FF, 0)
        gate_proj = jnp.dot(picked_rows, w_gate, preferred_element_type=jnp.float32)
        up_proj = jnp.dot(picked_rows, w_up, preferred_element_type=jnp.float32)
        hidden = (jax.nn.silu(gate_proj) * up_proj).astype(jnp.bfloat16)
        expert_out = jnp.dot(hidden, w_down, preferred_element_type=jnp.float32)
        row_weight = jnp.where(is_valid, weight_row[positions], jnp.float32(0.0))
        running = running.at[positions].add(row_weight[:, None] * expert_out)
        return running, None

    start_value = jnp.zeros((TOKENS, D), jnp.float32)
    combined, _ = lax.scan(one_expert, start_value, jnp.arange(EXP_WIN, dtype=jnp.int32))
    return combined.astype(jnp.bfloat16)
```

```python
import functools
import math

import jax
import jax.numpy as jnp
from jax import lax
from jax.experimental import pallas as pl
from jax.experimental.pallas import tpu as pltpu
from jax.sharding import PartitionSpec as P

FF = 2048
CAP = 2
CHUNKS = 4

route_scale = 2.5

MESH = pl.DeviceIdType.MESH
BF16 = jnp.bfloat16
F32 = jnp.float32


def moe_kernel(
    side,
    gs,
    tok_hbm,
    place_ref,
    mix_ref,
    wg_hbm,
    wu_hbm,
    wd_hbm,
    out_ref,
    tok,
    wg,
    wu,
    wd,
    send_y,
    recv_y,
    rows,
    oth,
    transit,
    gate_acc,
    up_acc,
    own_part,
    give,
    take,
    stage,
    from_right,
    from_left,
    oth_sum,
    transit_sum,
    send_r,
    recv_r,
    load_sem,
    ys,
    yr,
    xs,
    xr,
    os_,
    tr,
    ts,
    ps,
    pr,
    qs,
    qr,
    rs,
    rfr,
    rfl,
    tor,
    ttr,
    tts,
    zs,
    zr,
):
    chunks, width = oth.shape[0], oth.shape[2]
    quad = 2 * CAP
    reach = gs // 2
    slots = gs + 2 * reach
    last = gs - 1
    most = last + reach
    blk = lax.axis_index("blk")
    rep = lax.axis_index("rep")
    y = lax.div(blk, side)
    x = lax.rem(blk, side)
    w = lax.rem(x, gs)
    me = w + reach

    def at(yy, xx):
        return {"blk": yy * side + xx, "rep": rep}

    right = at(y, lax.rem(x + 1, side))
    left = at(y, lax.rem(x + side - 1, side))
    partner = {"rep": 1 - rep}

    def peer(d):
        return lax.rem(y + d, side)

    def remote(src, dst, send, recv, dev):
        return pltpu.make_async_remote_copy(
            src_ref=src, dst_ref=dst, send_sem=send, recv_sem=recv, device_id=dev, device_id_type=MESH
        )

    def arrived(dst, recv):
        remote(dst, dst, recv, recv, partner).wait_recv()

    loads = [
        pltpu.make_async_copy(src, dst, load_sem.at[k])
        for k, (src, dst) in enumerate(((tok_hbm, tok), (wg_hbm, wg), (wu_hbm, wu), (wd_hbm, wd)))
    ]
    for load in loads:
        load.start()

    barrier = pltpu.get_barrier_semaphore()
    for d in range(1, side):
        pl.semaphore_signal(barrier, inc=1, device_id=at(peer(d), x), device_id_type=MESH)
    for dev in (right, left, partner):
        pl.semaphore_signal(barrier, inc=1, device_id=dev, device_id_type=MESH)

    loads[0].wait()

    def cols(c):
        return pl.ds(pl.multiple_of(c * width, 128), width)

    def pack(c, _):
        packed = jnp.dot(place_ref[...], tok[:, cols(c)], preferred_element_type=F32)
        for yy in range(side):
            part = packed[yy * quad : (yy + 1) * quad].astype(BF16)
            send_y[yy, c] = part

            @pl.when(y == yy)
            def _():
                recv_y[yy, c] = part

        return 0

    lax.fori_loop(0, chunks, pack, 0)
    pl.semaphore_wait(barrier, side + 2)

    def y_copy(d, c):
        to = peer(d)
        return remote(send_y.at[to, c], recv_y.at[y, c], ys.at[to, c], yr.at[y, c], at(to, x))

    def right_copy(k, c):
        return remote(rows.at[0, k, c], rows.at[0, k, c], xs.at[0, k, c], xr.at[k, c], right)

    def left_copy(k, c):
        return remote(rows.at[0, k, c], rows.at[0, k, c], xs.at[1, k, c], xr.at[k, c], left)

    def partner_copy(k, c):
        return remote(rows.at[0, k, c], rows.at[1, k, c], ps.at[k, c], pr.at[k, c], partner)

    def oth_copies(c, act):
        for pos in range(gs):
            dev = left if pos < reach else right
            at_end = pos == 0 or pos == last
            slot = reach + gs if pos == 0 else reach - 1

            @pl.when(w == pos)
            def _():
                if at_end:
                    act(remote(oth.at[c], rows.at[0, slot, c], os_.at[c], xr.at[slot, c], dev))
                else:
                    act(remote(oth.at[c], transit.at[c], os_.at[c], tr.at[c], dev))

    def transit_copies(c, act, wait):
        for pos, dev, slot in ((0, left, slots - 1), (last, right, 0)):

            @pl.when(w == pos)
            def _():
                if wait:
                    arrived(transit.at[c], tr.at[c])
                act(remote(transit.at[c], rows.at[0, slot, c], ts.at[c], xr.at[slot, c], dev))

    def spread(k, c, to_right, to_left, act):
        if to_right:

            @pl.when(w < last)
            def _():
                act(right_copy(k, c))

        if to_left:

            @pl.when(w > 0)
            def _():
                act(left_copy(k, c))

        act(partner_copy(k, c))

    def start(copy):
        copy.start()

    def sent(copy):
        copy.wait_send()

    order = sorted(range(1, side), key=lambda d: -min(d, side - d))

    def send_out(c, _):
        for d in order:
            y_copy(d, c).start()
        return 0

    lax.fori_loop(0, chunks, send_out, 0)

    def own_step(c, _):
        for d in range(1, side):
            arrived(recv_y.at[peer(d), c], yr.at[peer(d), c])
        parts = [recv_y[j, c].astype(F32) for j in range(side)]
        oth[c] = jnp.concatenate([p[CAP:quad] for p in parts], axis=0).astype(BF16)
        rows[0, me, c] = jnp.concatenate([p[:CAP] for p in parts], axis=0).astype(BF16)
        oth_copies(c, start)
        spread(me, c, True, True, start)
        return 0

    lax.fori_loop(0, chunks, own_step, 0)

    def forward_step(t, _):
        i, c = lax.div(t, chunks) + 1, lax.rem(t, chunks)

        @pl.when(i == 1)
        def _():
            transit_copies(c, start, True)

        @pl.when(me - i >= 0)
        def _():
            arrived(rows.at[0, me - i, c], xr.at[me - i, c])
            spread(me - i, c, True, False, start)

        @pl.when(me + i < slots)
        def _():
            arrived(rows.at[0, me + i, c], xr.at[me + i, c])
            spread(me + i, c, False, True, start)

        return 0

    lax.fori_loop(0, most * chunks, forward_step, 0)

    for load in loads[1:]:
        load.wait()

    def partner_rows(t, _):
        k, c = lax.div(t, chunks), lax.rem(t, chunks)
        arrived(rows.at[1, k, c], pr.at[k, c])
        return 0

    lax.fori_loop(0, slots * chunks, partner_rows, 0)

    many = rows.shape[1] * rows.shape[3]
    gate_acc[...] = jnp.zeros_like(gate_acc)
    up_acc[...] = jnp.zeros_like(up_acc)

    def project(c, _):
        block = rows[:, :, pl.ds(c, 1)].reshape(2 * many, width)
        gate_acc[...] += jnp.dot(block, wg[cols(c), :], preferred_element_type=F32)
        up_acc[...] += jnp.dot(block, wu[cols(c), :], preferred_element_type=F32)
        return 0

    lax.fori_loop(0, chunks, project, 0)
    gate = gate_acc[...]
    hidden = (gate / (1.0 + jnp.exp(-gate)) * up_acc[...]).astype(BF16)

    def give_copy(c):
        return remote(give.at[c], take.at[c], qs.at[c], qr.at[c], partner)

    def down(c, _):
        part = jnp.dot(hidden, wd[:, cols(c)], preferred_element_type=F32)
        give[c] = part[many:].astype(BF16).reshape(give.shape[1:])
        own_part[c] = part[:many].reshape(own_part.shape[1:])
        give_copy(c).start()
        return 0

    lax.fori_loop(0, chunks, down, 0)

    def mine(k, c):
        return own_part[c, k] + take[c, k].astype(F32)

    def back_left(k, c, i, act):
        src = stage.at[k, c]

        @pl.when(w > 0)
        def _():
            act(remote(src, from_right.at[k, c], rs.at[k, c], rfr.at[k, c], left))

        @pl.when(jnp.logical_and(w == 0, i == 1))
        def _():
            act(remote(src, oth_sum.at[c], rs.at[k, c], tor.at[c], left))

        @pl.when(jnp.logical_and(w == 0, i > 1))
        def _():
            act(remote(src, transit_sum.at[c], rs.at[k, c], ttr.at[c], left))

    def back_right(k, c, i, act):
        src = stage.at[k, c]

        @pl.when(w < last)
        def _():
            act(remote(src, from_left.at[k, c], rs.at[k, c], rfl.at[k, c], right))

        @pl.when(jnp.logical_and(w == last, i == 1))
        def _():
            act(remote(src, oth_sum.at[c], rs.at[k, c], tor.at[c], right))

        @pl.when(jnp.logical_and(w == last, i > 1))
        def _():
            act(remote(src, transit_sum.at[c], rs.at[k, c], ttr.at[c], right))

    def back_step(t, _):
        i, c = most - lax.div(t, chunks), lax.rem(t, chunks)

        @pl.when(i == most)
        def _():
            arrived(take.at[c], qr.at[c])

        @pl.when(me - i >= 0)
        def _():
            k = me - i

            @pl.when(w == last)
            def _():
                stage[k, c] = mine(k, c).astype(BF16)

            @pl.when(w < last)
            def _():
                arrived(from_right.at[k, c], rfr.at[k, c])
                stage[k, c] = (mine(k, c) + from_right[k, c].astype(F32)).astype(BF16)

            back_left(k, c, i, start)

        @pl.when(me + i < slots)
        def _():
            k = me + i

            @pl.when(w == 0)
            def _():
                stage[k, c] = mine(k, c).astype(BF16)

            @pl.when(w > 0)
            def _():
                arrived(from_left.at[k, c], rfl.at[k, c])
                stage[k, c] = (mine(k, c) + from_left[k, c].astype(F32)).astype(BF16)

            back_right(k, c, i, start)

        return 0

    lax.fori_loop(0, most * chunks, back_step, 0)

    def transit_back(c, act, wait):
        for pos, dev in ((0, right), (last, left)):

            @pl.when(w == pos)
            def _():
                if wait:
                    arrived(transit_sum.at[c], ttr.at[c])
                act(remote(transit_sum.at[c], oth_sum.at[c], tts.at[c], tor.at[c], dev))

    def transit_loop(c, _):
        transit_back(c, start, True)
        return 0

    lax.fori_loop(0, chunks, transit_loop, 0)

    def z_copy(d, c):
        to = peer(d)
        return remote(send_r.at[to, c], recv_r.at[y, c], zs.at[to, c], zr.at[y, c], at(to, x))

    def root_step(c, _):
        gate_free = mine(me, c)
        own_part[c, me] = gate_free

        @pl.when(w < last)
        def _():
            arrived(from_right.at[me, c], rfr.at[me, c])
            own_part[c, me] += from_right[me, c].astype(F32)

        @pl.when(w > 0)
        def _():
            arrived(from_left.at[me, c], rfl.at[me, c])
            own_part[c, me] += from_left[me, c].astype(F32)

        arrived(oth_sum.at[c], tor.at[c])
        total = own_part[c, me]
        other = oth_sum[c].astype(F32)
        for j in range(side):
            pair = slice(j * CAP, (j + 1) * CAP)
            part = jnp.concatenate([total[pair], other[pair]], axis=0).astype(BF16)
            send_r[j, c] = part

            @pl.when(y == j)
            def _():
                recv_r[j, c] = part

        for d in order:
            z_copy(d, c).start()
        return 0

    lax.fori_loop(0, chunks, root_step, 0)

    mix = mix_ref[...]
    mix_hi = mix.astype(BF16)
    mix_lo = (mix - mix_hi.astype(F32)).astype(BF16)

    def combine(c, _):
        for d in range(1, side):
            arrived(recv_r.at[peer(d), c], zr.at[peer(d), c])
        block = jnp.concatenate([recv_r[j, c].astype(F32) for j in range(side)], axis=0).astype(BF16)
        total = jnp.dot(mix_hi, block, preferred_element_type=F32)
        total += jnp.dot(mix_lo, block, preferred_element_type=F32)
        out_ref[:, cols(c)] = total.astype(BF16)
        return 0

    lax.fori_loop(0, chunks, combine, 0)

    def drain(c, _):
        for d in range(1, side):
            y_copy(d, c).wait_send()
            z_copy(d, c).wait_send()
        oth_copies(c, sent)
        transit_copies(c, sent, False)
        transit_back(c, sent, False)
        spread(me, c, True, True, sent)
        give_copy(c).wait_send()
        return 0

    lax.fori_loop(0, chunks, drain, 0)

    def drain_far(t, _):
        i, c = lax.div(t, chunks) + 1, lax.rem(t, chunks)

        @pl.when(me - i >= 0)
        def _():
            spread(me - i, c, True, False, sent)
            back_left(me - i, c, i, sent)

        @pl.when(me + i < slots)
        def _():
            spread(me + i, c, False, True, sent)
            back_right(me + i, c, i, sent)

        return 0

    lax.fori_loop(0, most * chunks, drain_far, 0)


def shards(tokens, router_scores, expert_ids, gate_weight, up_weight, down_weight):
    blk_count = lax.axis_size("blk")
    rep_count = lax.axis_size("rep")
    count, model_width = tokens.shape
    units = gate_weight.shape[1]
    window = blk_count * rep_count * units // FF
    gs = blk_count // window
    side = math.isqrt(blk_count)
    per_row = side // gs
    own = lax.rem(lax.axis_index("blk"), side) // gs

    sigmoid_scores = jax.nn.sigmoid(router_scores)
    gate_values = route_scale * sigmoid_scores / jnp.sum(sigmoid_scores, axis=1, keepdims=True)
    spots = jnp.arange(window, dtype=jnp.int32)
    expert_of = spots // per_row * per_row + (spots % per_row + own) % per_row
    member = expert_ids[:, :, None] == expert_of[None, None, :]
    is_hit = jnp.any(member, axis=1)
    token_weight = jnp.sum(jnp.where(member, gate_values[:, :, None], jnp.float32(0.0)), axis=1)
    rank = jnp.cumsum(is_hit.astype(jnp.int32), axis=0) - 1
    placed = (rank[:, :, None] == jnp.arange(CAP, dtype=jnp.int32)) & is_hit[:, :, None]
    mix = jnp.where(placed, token_weight[:, :, None], jnp.float32(0.0)).reshape(count, window * CAP)
    place = placed.reshape(count, window * CAP).T.astype(BF16)

    chunks = CHUNKS
    width = model_width // chunks
    slots = 2 * gs
    unit = side * CAP
    quad = 2 * CAP
    vmem = pl.BlockSpec(memory_space=pltpu.VMEM)
    hbm = pl.BlockSpec(memory_space=pl.ANY)
    dma = pltpu.SemaphoreType.DMA
    return pl.pallas_call(
        functools.partial(moe_kernel, side, gs),
        out_shape=jax.ShapeDtypeStruct((count, model_width), BF16),
        in_specs=[hbm, vmem, vmem, hbm, hbm, hbm],
        out_specs=vmem,
        scratch_shapes=[
            pltpu.VMEM((count, model_width), BF16),
            pltpu.VMEM(gate_weight.shape, BF16),
            pltpu.VMEM(up_weight.shape, BF16),
            pltpu.VMEM(down_weight.shape, BF16),
            pltpu.VMEM((side, chunks, quad, width), BF16),
            pltpu.VMEM((side, chunks, quad, width), BF16),
            pltpu.VMEM((2, slots, chunks, unit, width), BF16),
            pltpu.VMEM((chunks, unit, width), BF16),
            pltpu.VMEM((chunks, unit, width), BF16),
            pltpu.VMEM((2 * slots * unit, units), F32),
            pltpu.VMEM((2 * slots * unit, units), F32),
            pltpu.VMEM((chunks, slots, unit, width), F32),
            pltpu.VMEM((chunks, slots, unit, width), BF16),
            pltpu.VMEM((chunks, slots, unit, width), BF16),
            pltpu.VMEM((slots, chunks, unit, width), BF16),
            pltpu.VMEM((slots, chunks, unit, width), BF16),
            pltpu.VMEM((slots, chunks, unit, width), BF16),
            pltpu.VMEM((chunks, unit, width), BF16),
            pltpu.VMEM((chunks, unit, width), BF16),
            pltpu.VMEM((side, chunks, quad, width), BF16),
            pltpu.VMEM((side, chunks, quad, width), BF16),
            dma((4,)),
            dma((side, chunks)),
            dma((side, chunks)),
            dma((2, slots, chunks)),
            dma((slots, chunks)),
            dma((chunks,)),
            dma((chunks,)),
            dma((chunks,)),
            dma((slots, chunks)),
            dma((slots, chunks)),
            dma((chunks,)),
            dma((chunks,)),
            dma((slots, chunks)),
            dma((slots, chunks)),
            dma((slots, chunks)),
            dma((chunks,)),
            dma((chunks,)),
            dma((chunks,)),
            dma((side, chunks)),
            dma((side, chunks)),
        ],
        compiler_params=pltpu.CompilerParams(
            collective_id=0, has_side_effects=True, vmem_limit_bytes=58 * 1024 * 1024
        ),
    )(tokens, place, mix, gate_weight, up_weight, down_weight)


def solution(mesh):
    placed = (
        P(("groups", "blk", "rep"), None),
        P(("groups", "blk", "rep"), None),
        P(("groups", "blk", "rep"), None),
        P(None, ("blk", "rep")),
        P(None, ("blk", "rep")),
        P(("blk", "rep"), None),
    )
    return jax.shard_map(
        shards,
        mesh=mesh,
        in_specs=placed,
        out_specs=P(("groups", "blk", "rep"), None),
        check_vma=False,
    )
```

```python
import functools
import math

import jax
import jax.numpy as jnp
from jax import lax
from jax.experimental import pallas as pl
from jax.experimental.pallas import tpu as pltpu
from jax.sharding import PartitionSpec as P

FF = 2048
CAP = 2
CHUNKS = 4

BATCHES = ((0, 0), (0, 1), (1, 1), (1, 0))
KINDS = "OFLGDBVRC"
ORDER = (
    0, 10, 201, 101, 111, 211, 202, 102, 20, 212, 112, 103, 203, 204, 113, 104, 121, 30,
    105, 213, 221, 122, 205, 114, 300, 231, 400, 131, 214, 222, 232, 605, 115, 123, 215, 505,
    132, 223, 310, 604, 233, 124, 410, 133, 224, 234, 504, 603, 503, 125, 615, 134, 614, 515,
    225, 235, 320, 514, 602, 502, 513, 420, 613, 135, 330, 625, 525, 601, 524, 430, 624, 512,
    612, 535, 635, 501, 623, 534, 634, 523, 611, 511, 633, 533, 522, 622, 700, 710, 532, 632,
    521, 621, 531, 631, 810, 800, 720, 730, 820, 830,
)

route_scale = 2.5

MESH = pl.DeviceIdType.MESH
BF16 = jnp.bfloat16
F32 = jnp.float32


def moe_kernel(
    side,
    gs,
    scores_hbm,
    ids_hbm,
    tok_hbm,
    wg_hbm,
    wu_hbm,
    wd_hbm,
    out_ref,
    scores_ref,
    ids_ref,
    tok,
    wg,
    wu,
    wd,
    mixes,
    send_y,
    recv_y,
    rows,
    oth,
    hidden,
    own_part,
    give,
    take,
    stage,
    from_right,
    from_left,
    oth_sum,
    send_r,
    recv_r,
    out_acc,
    load_sem,
    ys,
    yr,
    xs,
    xr,
    os_,
    ps,
    pr,
    qs,
    qr,
    rs,
    rf,
    rroot,
    tor,
    zs,
    zr,
):
    batches, unit, depth = oth.shape
    count, top = tok.shape[0], ids_ref.shape[0]
    width = depth // CHUNKS
    per_row = side // gs
    half = side // 2
    reach = gs // 2
    slots = gs + 2 * reach
    last = gs - 1
    most = last + reach
    blk = lax.axis_index("blk")
    rep = lax.axis_index("rep")
    y = lax.div(blk, side)
    x = lax.rem(blk, side)
    w = lax.rem(x, gs)
    me = w + reach
    my_half, my_m = lax.div(y, half), lax.rem(y, half)

    def at(yy, xx):
        return {"blk": yy * side + lax.rem(xx + side, side), "rep": rep}

    right = at(y, x + 1)
    left = at(y, x - 1)
    partner = {"rep": 1 - rep}

    def row_of(rel, m):
        return lax.rem(my_half + rel, 2) * half + m

    def remote(src, dst, send, recv, dev):
        return pltpu.make_async_remote_copy(
            src_ref=src, dst_ref=dst, send_sem=send, recv_sem=recv, device_id=dev, device_id_type=MESH
        )

    def arrived(ref, recv):
        remote(ref, ref, recv, recv, partner).wait_recv()

    def sent(ref, send):
        remote(ref, ref, send, send, partner).wait_send()

    def per_cols(body):
        def step(c, _):
            body(pl.ds(pl.multiple_of(c * width, 128), width))
            return 0

        lax.fori_loop(0, CHUNKS, step, 0)

    load_tok = pltpu.make_async_copy(tok_hbm, tok, load_sem.at[0])
    loads = [
        pltpu.make_async_copy(src, dst, load_sem.at[k + 1])
        for k, (src, dst) in enumerate(((wg_hbm, wg), (wu_hbm, wu), (wd_hbm, wd)))
    ]
    tables = [
        pltpu.make_async_copy(src, dst, load_sem.at[4 + k])
        for k, (src, dst) in enumerate(((scores_hbm, scores_ref), (ids_hbm, ids_ref)))
    ]
    for load in tables:
        load.start()
    load_tok.start()

    barrier = pltpu.get_barrier_semaphore()
    for d in range(1, side):
        pl.semaphore_signal(barrier, inc=1, device_id=at(lax.rem(y + d, side), x), device_id_type=MESH)
    for hop in range(1, reach + 1):
        for dev in (at(y, x + hop), at(y, x - hop)):
            pl.semaphore_signal(barrier, inc=1, device_id=dev, device_id_type=MESH)
    pl.semaphore_signal(barrier, inc=1, device_id=partner, device_id_type=MESH)

    for load in tables:
        load.wait()
    spots = side * per_row
    sigmoid = 1.0 / (1.0 + jnp.exp(-scores_ref[...]))
    gates = route_scale * sigmoid / jnp.sum(sigmoid, axis=0, keepdims=True)
    spot = lax.broadcasted_iota(jnp.int32, (spots, count), 0)
    of_half = lax.rem(lax.div(spot, half * per_row) + my_half, 2)
    of_row = of_half * half + lax.rem(lax.div(spot, per_row), half)
    of_expert = of_row * per_row + lax.rem(lax.rem(spot, per_row) + lax.div(x, gs), per_row)
    ids = ids_ref[...]
    weight = jnp.zeros((spots, count), F32)
    hit = jnp.zeros((spots, count), F32)
    for k in range(top):
        same = ids[k : k + 1] == of_expert
        weight += jnp.where(same, gates[k : k + 1], 0.0)
        hit += jnp.where(same, 1.0, 0.0)
    before = lax.broadcasted_iota(jnp.int32, (count, count), 0) < lax.broadcasted_iota(
        jnp.int32, (count, count), 1
    )
    rank = jnp.dot(hit.astype(BF16), jnp.where(before, 1.0, 0.0).astype(BF16), preferred_element_type=F32)
    placed = [jnp.where(rank == s, hit, 0.0) for s in range(CAP)]

    n = half * per_row
    eye = (
        lax.broadcasted_iota(jnp.int32, (n, n), 0) == lax.broadcasted_iota(jnp.int32, (n, n), 1)
    ).astype(F32).astype(BF16)
    for b, (s, rel) in enumerate(BATCHES):
        mix = (placed[s] * weight)[rel * n : (rel + 1) * n]
        mix_hi = mix.astype(BF16)
        mix_lo = (mix - mix_hi.astype(F32)).astype(BF16)
        turned = [
            lax.dot_general(m, eye, (((0,), (0,)), ((), ())), preferred_element_type=F32)
            for m in (mix_hi, mix_lo)
        ]
        mixes[b] = jnp.concatenate(turned, axis=1).astype(BF16)

    load_tok.wait()
    for load in loads:
        load.start()

    for s in range(CAP):
        choose = placed[s].astype(BF16)

        def pack(cols):
            packed = jnp.dot(choose, tok[:, cols], preferred_element_type=F32)
            for p in range(side):
                send_y[s * side + p, :, cols] = packed[p * per_row : (p + 1) * per_row].astype(BF16)

        per_cols(pack)

    pl.semaphore_wait(barrier, side + 2 * reach)

    def exchange(b, source, first, into, send, recv):
        s, rel = BATCHES[b]
        order = (2, 1, 3, 0) if half == 4 else range(half)
        for m in order:
            to = row_of(rel, m)
            src, dst = source.at[first + m], into.at[b * half + my_m]

            def away():
                remote(src, dst, send.at[0], recv.at[b], at(to, x)).start()

            if rel == 0:
                pl.when(my_m != m)(away)

                @pl.when(my_m == m)
                def _():
                    pltpu.make_async_copy(src, dst, recv.at[b]).start()

            else:
                away()

    def forward(b, k, to_right, to_left):
        at_k = b * slots + k
        ref = rows.at[0, at_k]
        if to_right:

            @pl.when(w < last)
            def _():
                remote(ref, ref, xs.at[0], xr.at[at_k], right).start()

        if to_left:

            @pl.when(w > 0)
            def _():
                remote(ref, ref, xs.at[1], xr.at[at_k], left).start()

        remote(ref, rows.at[1, at_k], ps.at[0], pr.at[b], partner).start()

    def y_task(b, _):
        s, rel = BATCHES[b]
        exchange(b, send_y, s * side + rel * half, recv_y, ys, yr)

    def own_task(b, _):
        arrived(recv_y.at[pl.ds(b * half, half)], yr.at[b])

        def body(cols):
            parts = [recv_y[b * half + m, :, cols].astype(F32) for m in range(half)]
            oth[b, :, cols] = jnp.concatenate([p[1:2] for p in parts], axis=0).astype(BF16)
            rows[0, b * slots + me, :, cols] = jnp.concatenate([p[:1] for p in parts], axis=0).astype(BF16)

        per_cols(body)
        near = w < reach
        hop = jnp.where(near, -(w + 1), gs - w)
        slot = b * slots + jnp.where(near, reach + gs + w, w - gs + reach)
        remote(oth.at[b], rows.at[0, slot], os_.at[0], xr.at[slot], at(y, x + hop)).start()
        forward(b, me, True, True)

    def forward_right_task(b, i):
        @pl.when(me - i >= 0)
        def _():
            arrived(rows.at[0, b * slots + me - i], xr.at[b * slots + me - i])
            forward(b, me - i, True, False)

    def forward_left_task(b, i):
        @pl.when(me + i < slots)
        def _():
            arrived(rows.at[0, b * slots + me + i], xr.at[b * slots + me + i])
            forward(b, me + i, False, True)

    many = slots * unit

    loaded = []

    def gate_task(b, _):
        if not loaded:
            loaded.append(b)
            for load in loads:
                load.wait()
        arrived(rows.at[1, pl.ds(b * slots, slots)], pr.at[b])
        block = rows[:, b * slots : (b + 1) * slots].reshape(2 * many, depth)
        gate = jnp.dot(block, wg[...], preferred_element_type=F32)
        up = jnp.dot(block, wu[...], preferred_element_type=F32)
        hidden[...] = (gate / (1.0 + jnp.exp(-gate)) * up).astype(BF16)

    def down_task(b, _):
        def body(cols):
            part = jnp.dot(hidden[...], wd[:, cols], preferred_element_type=F32)
            give[b, :, :, cols] = part[many:].astype(BF16).reshape(slots, unit, width)
            own_part[b, :, :, cols] = part[:many].reshape(slots, unit, width)

        per_cols(body)
        remote(give.at[b], take.at[b], qs.at[0], qr.at[b], partner).start()

    took = []

    def back_task(to_left, b, i):
        if b not in took:
            took.append(b)
            arrived(take.at[b], qr.at[b])

        if True:
            k = me - i if to_left else me + i
            at_k = b * slots + k
            leaf = w == last if to_left else w == 0
            at_end = w == 0 if to_left else w == last
            near = left if to_left else right
            buf = from_right if to_left else from_left
            recv = rroot.at[b] if i == 1 and not to_left else rf.at[at_k]

            @pl.when(k >= 0 if to_left else k < slots)
            def _():
                @pl.when(leaf)
                def _():
                    def body(cols):
                        total = own_part[b, k, :, cols] + take[b, k, :, cols].astype(F32)
                        stage[at_k, :, cols] = total.astype(BF16)

                    per_cols(body)

                @pl.when(jnp.logical_not(leaf))
                def _():
                    arrived(buf.at[at_k], rf.at[at_k])

                    def body(cols):
                        total = own_part[b, k, :, cols] + take[b, k, :, cols].astype(F32)
                        total += buf[at_k, :, cols].astype(F32)
                        stage[at_k, :, cols] = total.astype(BF16)

                    per_cols(body)

                src = stage.at[at_k]

                @pl.when(jnp.logical_not(at_end))
                def _():
                    remote(src, buf.at[at_k], rs.at[0], recv, near).start()

                @pl.when(at_end)
                def _():
                    far = at(y, x - i if to_left else x + i)
                    remote(src, oth_sum.at[b], rs.at[0], tor.at[b], far).start()

    def root_task(b, _):
        at_me = b * slots + me

        def body(cols):
            own_part[b, me, :, cols] += take[b, me, :, cols].astype(F32)

        per_cols(body)

        @pl.when(w < last)
        def _():
            arrived(from_right.at[at_me], rf.at[at_me])

            def body(cols):
                own_part[b, me, :, cols] += from_right[at_me, :, cols].astype(F32)

            per_cols(body)

        @pl.when(w > 0)
        def _():
            arrived(from_left.at[at_me], rroot.at[b])

            def body(cols):
                own_part[b, me, :, cols] += from_left[at_me, :, cols].astype(F32)

            per_cols(body)

        arrived(oth_sum.at[b], tor.at[b])

        def split(cols):
            total = own_part[b, me, :, cols]
            other = oth_sum[b, :, cols].astype(F32)
            for m in range(half):
                pair = jnp.concatenate([total[m : m + 1], other[m : m + 1]], axis=0)
                send_r[b * half + m, :, cols] = pair.astype(BF16)

        per_cols(split)
        exchange(b, send_r, b * half, recv_r, zs, zr)

    combined = []

    def combine_task(b, _):
        arrived(recv_r.at[pl.ds(b * half, half)], zr.at[b])
        mix = mixes[b]
        begin, end = not combined, len(combined) == batches - 1
        combined.append(b)

        def body(cols):
            parts = [recv_r[b * half + m, :, cols].astype(F32) for m in range(half)]
            block = jnp.concatenate(parts + parts, axis=0).astype(BF16)
            total = jnp.dot(mix, block, preferred_element_type=F32)
            if not begin:
                total += out_acc[:, cols]
            if end:
                out_ref[:, cols] = total.astype(BF16)
            else:
                out_acc[:, cols] = total

        per_cols(body)

    tasks = (
        own_task,
        forward_right_task,
        forward_left_task,
        gate_task,
        down_task,
        functools.partial(back_task, True),
        functools.partial(back_task, False),
        root_task,
        combine_task,
    )
    for b in range(batches):
        y_task(b, 0)
    for code in ORDER:
        kind, b, i = code // 100, code // 10 % 10, code % 10
        with jax.named_scope(f"{KINDS[kind]}{b}{i}"):
            tasks[kind](b, i)

    with jax.named_scope("drain"):
        away = CAP * (side - 1)
        sent(send_y.at[pl.ds(0, away)], ys.at[0])
        sent(send_r.at[pl.ds(0, away)], zs.at[0])
        sent(oth, os_.at[0])
        sent(rows.at[0], ps.at[0])
        sent(give, qs.at[0])
        sent(stage.at[pl.ds(0, batches * (slots - 1))], rs.at[0])
        for pos in range(gs):

            @pl.when(w == pos)
            def _():
                if pos < last:
                    sent(rows.at[0, pl.ds(0, batches * (pos + reach + 1))], xs.at[0])
                if pos > 0:
                    sent(rows.at[0, pl.ds(0, batches * (slots - reach - pos))], xs.at[1])


def shards(tokens, router_scores, expert_ids, gate_weight, up_weight, down_weight):
    blk_count = lax.axis_size("blk")
    rep_count = lax.axis_size("rep")
    count, depth = tokens.shape
    units = gate_weight.shape[1]
    window = blk_count * rep_count * units // FF
    gs = blk_count // window
    side = math.isqrt(blk_count)
    per_row = side // gs

    batches = len(BATCHES)
    slots = 2 * gs
    unit = side // 2
    many = slots * unit
    vmem = pl.BlockSpec(memory_space=pltpu.VMEM)
    hbm = pl.BlockSpec(memory_space=pltpu.HBM)
    dma = pltpu.SemaphoreType.DMA
    pieces = pltpu.VMEM((CAP * side, per_row, depth), BF16)
    blocks = pltpu.VMEM((batches * slots, unit, depth), BF16)
    parts = (batches, slots, unit, depth)
    single = pltpu.VMEM((batches, unit, depth), BF16)
    large = [
        pltpu.with_memory_space_constraint(a, pltpu.HBM)
        for a in (router_scores.T, expert_ids.T, tokens, gate_weight, up_weight, down_weight)
    ]
    return pl.pallas_call(
        functools.partial(moe_kernel, side, gs),
        out_shape=jax.ShapeDtypeStruct((count, depth), BF16),
        in_specs=[hbm] * len(large),
        out_specs=vmem,
        scratch_shapes=[
            pltpu.VMEM(router_scores.shape[::-1], F32),
            pltpu.VMEM(expert_ids.shape[::-1], jnp.int32),
            pltpu.VMEM((count, depth), BF16),
            pltpu.VMEM(gate_weight.shape, BF16),
            pltpu.VMEM(up_weight.shape, BF16),
            pltpu.VMEM(down_weight.shape, BF16),
            pltpu.VMEM((batches, count, side * per_row), BF16),
            pieces,
            pieces,
            pltpu.VMEM((2, batches * slots, unit, depth), BF16),
            single,
            pltpu.VMEM((2 * many, units), BF16),
            pltpu.VMEM(parts, F32),
            pltpu.VMEM(parts, BF16),
            pltpu.VMEM(parts, BF16),
            blocks,
            blocks,
            blocks,
            single,
            pieces,
            pieces,
            pltpu.VMEM((count, depth), F32),
            dma((6,)),
            dma((1,)),
            dma((batches,)),
            dma((2,)),
            dma((batches * slots,)),
            dma((1,)),
            dma((1,)),
            dma((batches,)),
            dma((1,)),
            dma((batches,)),
            dma((1,)),
            dma((batches * slots,)),
            dma((batches,)),
            dma((batches,)),
            dma((1,)),
            dma((batches,)),
        ],
        compiler_params=pltpu.CompilerParams(
            collective_id=0, has_side_effects=True, vmem_limit_bytes=44 * 1024 * 1024
        ),
    )(*large)


def solution(mesh):
    placed = (
        P(("groups", "blk", "rep"), None),
        P(("groups", "blk", "rep"), None),
        P(("groups", "blk", "rep"), None),
        P(None, ("blk", "rep")),
        P(None, ("blk", "rep")),
        P(("blk", "rep"), None),
    )
    return jax.shard_map(
        shards,
        mesh=mesh,
        in_specs=placed,
        out_specs=P(("groups", "blk", "rep"), None),
        check_vma=False,
    )
```

```python
import functools
import math

import jax
import jax.numpy as jnp
from jax import lax
from jax.experimental import pallas as pl
from jax.experimental.pallas import tpu as pltpu
from jax.sharding import PartitionSpec as P

FF = 2048
CAP = 2
CHUNKS = 4

BATCHES = ((0, 0), (0, 1), (1, 1), (1, 0))
KINDS = "OFLGDBVRC"
ORDER = (
    0, 10, 101, 20, 102, 201, 111, 211, 103, 121, 202, 112, 203, 122, 204, 212, 205, 30,
    113, 300, 123, 400, 213, 214, 131, 221, 605, 215, 222, 231, 310, 132, 223, 410, 232, 604,
    615, 224, 233, 133, 503, 603, 614, 225, 234, 602, 320, 613, 502, 420, 612, 235, 601, 330,
    501, 625, 430, 513, 624, 635, 623, 512, 700, 634, 523, 622, 511, 633, 611, 533, 522, 800,
    632, 532, 621, 521, 710, 631, 531, 720, 730, 810, 820, 830,
)

route_scale = 2.5

MESH = pl.DeviceIdType.MESH
BF16 = jnp.bfloat16
F32 = jnp.float32


def moe_kernel(
    side,
    gs,
    scores_hbm,
    ids_hbm,
    tok_hbm,
    wg_hbm,
    wu_hbm,
    wd_hbm,
    out_ref,
    scores_ref,
    ids_ref,
    tok,
    wg,
    wu,
    wd,
    mixes,
    send_y,
    recv_y,
    rows,
    oth,
    hidden,
    own_part,
    give,
    take,
    stage,
    came,
    oth_sum,
    send_r,
    recv_r,
    out_acc,
    load_sem,
    ys,
    yr,
    xs,
    xr,
    os_,
    ps,
    pr,
    qs,
    qr,
    rs,
    rf,
    rroot,
    tor,
    zs,
    zr,
):
    batches, unit, depth = oth.shape
    count, top = tok.shape[0], ids_ref.shape[0]
    width = depth // CHUNKS
    per_row = side // gs
    half = side // 2
    reach = gs // 2
    slots = gs + 2 * reach
    last = gs - 1
    most = last + reach
    blk = lax.axis_index("blk")
    rep = lax.axis_index("rep")
    y = lax.div(blk, side)
    x = lax.rem(blk, side)
    w = lax.rem(x, gs)
    me = w + reach
    my_half, my_m = lax.rem(y, 2), lax.div(y, 2)

    def at(yy, xx):
        return {"blk": yy * side + lax.rem(xx + side, side), "rep": rep}

    sign = jnp.where(w < reach, 1, -1)
    inner = jnp.logical_and(w > 0, w < last)
    up_side = jnp.where(w < reach, 0, 1)
    depth_in = jnp.minimum(w, last - w)
    up = at(y, x + sign)
    down = at(y, x - sign)
    partner = {"rep": 1 - rep}

    def row_of(rel, m):
        return m * 2 + lax.rem(my_half + rel, 2)

    def remote(src, dst, send, recv, dev):
        return pltpu.make_async_remote_copy(
            src_ref=src, dst_ref=dst, send_sem=send, recv_sem=recv, device_id=dev, device_id_type=MESH
        )

    def arrived(ref, recv):
        remote(ref, ref, recv, recv, partner).wait_recv()

    def sent(ref, send):
        remote(ref, ref, send, send, partner).wait_send()

    def per_cols(body):
        def step(c, _):
            body(pl.ds(pl.multiple_of(c * width, 128), width))
            return 0

        lax.fori_loop(0, CHUNKS, step, 0)

    load_tok = pltpu.make_async_copy(tok_hbm, tok, load_sem.at[0])
    loads = [
        pltpu.make_async_copy(src, dst, load_sem.at[k + 1])
        for k, (src, dst) in enumerate(((wg_hbm, wg), (wu_hbm, wu), (wd_hbm, wd)))
    ]
    tables = [
        pltpu.make_async_copy(src, dst, load_sem.at[4 + k])
        for k, (src, dst) in enumerate(((scores_hbm, scores_ref), (ids_hbm, ids_ref)))
    ]
    for load in tables:
        load.start()
    load_tok.start()

    barrier = pltpu.get_barrier_semaphore()
    for d in range(1, side):
        pl.semaphore_signal(barrier, inc=1, device_id=at(lax.rem(y + d, side), x), device_id_type=MESH)
    for hop in range(1, reach + 1):
        for dev in (at(y, x + hop), at(y, x - hop)):
            pl.semaphore_signal(barrier, inc=1, device_id=dev, device_id_type=MESH)
    pl.semaphore_signal(barrier, inc=1, device_id=partner, device_id_type=MESH)

    for load in tables:
        load.wait()
    spots = side * per_row
    sigmoid = 1.0 / (1.0 + jnp.exp(-scores_ref[...]))
    gates = route_scale * sigmoid / jnp.sum(sigmoid, axis=0, keepdims=True)
    spot = lax.broadcasted_iota(jnp.int32, (spots, count), 0)
    of_half = lax.rem(lax.div(spot, half * per_row) + my_half, 2)
    of_row = lax.rem(lax.div(spot, per_row), half) * 2 + of_half
    of_expert = of_row * per_row + lax.rem(lax.rem(spot, per_row) + lax.div(x, gs), per_row)
    ids = ids_ref[...]
    weight = jnp.zeros((spots, count), F32)
    hit = jnp.zeros((spots, count), F32)
    for k in range(top):
        same = ids[k : k + 1] == of_expert
        weight += jnp.where(same, gates[k : k + 1], 0.0)
        hit += jnp.where(same, 1.0, 0.0)
    before = lax.broadcasted_iota(jnp.int32, (count, count), 0) < lax.broadcasted_iota(
        jnp.int32, (count, count), 1
    )
    rank = jnp.dot(hit.astype(BF16), jnp.where(before, 1.0, 0.0).astype(BF16), preferred_element_type=F32)
    placed = [jnp.where(rank == s, hit, 0.0) for s in range(CAP)]

    n = half * per_row
    eye = (
        lax.broadcasted_iota(jnp.int32, (n, n), 0) == lax.broadcasted_iota(jnp.int32, (n, n), 1)
    ).astype(F32).astype(BF16)
    for b, (s, rel) in enumerate(BATCHES):
        mix = (placed[s] * weight)[rel * n : (rel + 1) * n]
        mix_hi = mix.astype(BF16)
        mix_lo = (mix - mix_hi.astype(F32)).astype(BF16)
        turned = [
            lax.dot_general(m, eye, (((0,), (0,)), ((), ())), preferred_element_type=F32)
            for m in (mix_hi, mix_lo)
        ]
        mixes[b] = jnp.concatenate(turned, axis=1).astype(BF16)

    load_tok.wait()
    for load in loads:
        load.start()

    for s in range(CAP):
        choose = placed[s].astype(BF16)

        def pack(cols):
            packed = jnp.dot(choose, tok[:, cols], preferred_element_type=F32)
            for p in range(side):
                send_y[s * side + p, :, cols] = packed[p * per_row : (p + 1) * per_row].astype(BF16)

        per_cols(pack)

    pl.semaphore_wait(barrier, side + 2 * reach)

    def exchange(b, source, first, into, send, recv):
        s, rel = BATCHES[b]
        order = (2, 1, 3, 0) if half == 4 else range(half)
        for m in order:
            to = row_of(rel, m)
            src, dst = source.at[first + m], into.at[b * half + my_m]

            def away():
                remote(src, dst, send.at[0], recv.at[b], at(to, x)).start()

            if rel == 0:
                pl.when(my_m != m)(away)

                @pl.when(my_m == m)
                def _():
                    pltpu.make_async_copy(src, dst, recv.at[b]).start()

            else:
                away()

    def forward(b, k, to_up, to_down):
        at_k = b * slots + k
        ref = rows.at[0, at_k]
        if to_up:
            remote(ref, ref, xs.at[0], xr.at[at_k], up).start()

        if to_down:

            @pl.when(inner)
            def _():
                remote(ref, ref, xs.at[1], xr.at[at_k], down).start()

        remote(ref, rows.at[1, at_k], ps.at[0], pr.at[b], partner).start()

    def y_task(b, _):
        s, rel = BATCHES[b]
        exchange(b, send_y, s * side + rel * half, recv_y, ys, yr)

    def own_task(b, _):
        arrived(recv_y.at[pl.ds(b * half, half)], yr.at[b])

        def body(cols):
            parts = [recv_y[b * half + m, :, cols].astype(F32) for m in range(half)]
            oth[b, :, cols] = jnp.concatenate([p[1:2] for p in parts], axis=0).astype(BF16)
            rows[0, b * slots + me, :, cols] = jnp.concatenate([p[:1] for p in parts], axis=0).astype(BF16)

        per_cols(body)
        near = w < reach
        hop = jnp.where(near, -(w + 1), gs - w)
        slot = b * slots + jnp.where(near, reach + gs + w, w - gs + reach)
        remote(oth.at[b], rows.at[0, slot], os_.at[0], xr.at[slot], at(y, x + hop)).start()
        forward(b, me, True, True)

    def when_far(i, most_in, body):
        if i > most_in:
            pl.when(inner)(body)
        else:
            body()

    def forward_up_task(b, i):
        def body():
            k = me - sign * i
            arrived(rows.at[0, b * slots + k], xr.at[b * slots + k])
            forward(b, k, True, False)

        when_far(i, reach, body)

    def forward_down_task(b, i):
        def body():
            k = me + sign * i
            arrived(rows.at[0, b * slots + k], xr.at[b * slots + k])
            forward(b, k, False, True)

        if i == most:
            pl.when(jnp.logical_not(inner))(body)
        else:
            body()

    many = slots * unit

    loaded = []

    def gate_task(b, _):
        if not loaded:
            loaded.append(b)
            for load in loads:
                load.wait()
        arrived(rows.at[1, pl.ds(b * slots, slots)], pr.at[b])
        block = rows[:, b * slots : (b + 1) * slots].reshape(2 * many, depth)
        gate = jnp.dot(block, wg[...], preferred_element_type=F32)
        up = jnp.dot(block, wu[...], preferred_element_type=F32)
        hidden[...] = (gate / (1.0 + jnp.exp(-gate)) * up).astype(BF16)

    def down_task(b, _):
        def body(cols):
            part = jnp.dot(hidden[...], wd[:, cols], preferred_element_type=F32)
            give[b, :, :, cols] = part[many:].astype(BF16).reshape(slots, unit, width)
            own_part[b, :, :, cols] = part[:many].reshape(slots, unit, width)
            ours, theirs = give.at[b, :, :, cols], take.at[b, :, :, cols]
            remote(ours, theirs, qs.at[0], qr.at[b], partner).start()

        per_cols(body)

    took = []

    def partial_sum(b, k, side_in, at_in):
        at_k = b * slots + k

        def body(cols):
            total = own_part[b, k, :, cols] + take[b, k, :, cols].astype(F32)
            if at_in:
                total += came.at[side_in][at_k, :, cols].astype(F32)
            stage[at_k, :, cols] = total.astype(BF16)

        if at_in:
            arrived(came.at[side_in, at_k], rf.at[at_k])
        per_cols(body)

    def taken(b):
        if b not in took:
            took.append(b)
            arrived(take.at[b], qr.at[b])

    def back_down_task(b, i):
        taken(b)

        def body():
            k = me - sign * i
            at_k = b * slots + k
            partial_sum(b, k, up_side, True)
            src = stage.at[at_k]
            recv = rroot.at[up_side, b] if i == 1 else rf.at[at_k]

            @pl.when(inner)
            def _():
                remote(src, came.at[up_side, at_k], rs.at[0], recv, down).start()

            @pl.when(jnp.logical_not(inner))
            def _():
                remote(src, oth_sum.at[b], rs.at[0], tor.at[b], at(y, x - sign * i)).start()

        when_far(i, reach, body)

    def back_up_task(b, i):
        taken(b)
        k = me + sign * i
        at_k = b * slots + k
        recv = rroot.at[1 - up_side, b] if i == 1 else rf.at[at_k]

        @pl.when(jnp.logical_not(inner))
        def _():
            partial_sum(b, k, 1 - up_side, False)

        if i < most:

            @pl.when(inner)
            def _():
                partial_sum(b, k, 1 - up_side, True)

        def body():
            remote(stage.at[at_k], came.at[1 - up_side, at_k], rs.at[0], recv, up).start()

        if i == most:
            pl.when(jnp.logical_not(inner))(body)
        else:
            body()

    def root_task(b, _):
        at_me = b * slots + me

        def body(cols):
            own_part[b, me, :, cols] += take[b, me, :, cols].astype(F32)

        per_cols(body)

        def add(side_in):
            arrived(came.at[side_in, at_me], rroot.at[side_in, b])

            def body(cols):
                own_part[b, me, :, cols] += came.at[side_in][at_me, :, cols].astype(F32)

            per_cols(body)

        add(up_side)
        pl.when(inner)(lambda: add(1 - up_side))
        arrived(oth_sum.at[b], tor.at[b])

        def split(cols):
            total = own_part[b, me, :, cols]
            other = oth_sum[b, :, cols].astype(F32)
            for m in range(half):
                pair = jnp.concatenate([total[m : m + 1], other[m : m + 1]], axis=0)
                send_r[b * half + m, :, cols] = pair.astype(BF16)

        per_cols(split)
        exchange(b, send_r, b * half, recv_r, zs, zr)

    combined = []

    def combine_task(b, _):
        arrived(recv_r.at[pl.ds(b * half, half)], zr.at[b])
        mix = mixes[b]
        begin, end = not combined, len(combined) == batches - 1
        combined.append(b)

        def body(cols):
            parts = [recv_r[b * half + m, :, cols].astype(F32) for m in range(half)]
            block = jnp.concatenate(parts + parts, axis=0).astype(BF16)
            total = jnp.dot(mix, block, preferred_element_type=F32)
            if not begin:
                total += out_acc[:, cols]
            if end:
                out_ref[:, cols] = total.astype(BF16)
            else:
                out_acc[:, cols] = total

        per_cols(body)

    tasks = (
        own_task,
        forward_up_task,
        forward_down_task,
        gate_task,
        down_task,
        back_down_task,
        back_up_task,
        root_task,
        combine_task,
    )
    for b in range(batches):
        y_task(b, 0)
    for code in ORDER:
        kind, b, i = code // 100, code // 10 % 10, code % 10
        with jax.named_scope(f"{KINDS[kind]}{b}{i}"):
            tasks[kind](b, i)

    with jax.named_scope("drain"):
        away = CAP * (side - 1)
        sent(send_y.at[pl.ds(0, away)], ys.at[0])
        sent(send_r.at[pl.ds(0, away)], zs.at[0])
        sent(oth, os_.at[0])
        sent(rows.at[0], ps.at[0])
        sent(give, qs.at[0])
        sent(stage.at[pl.ds(0, batches * (slots - 1))], rs.at[0])
        for pos in range(reach):

            @pl.when(depth_in == pos)
            def _():
                sent(rows.at[0, pl.ds(0, batches * (pos + reach + 1))], xs.at[0])
                if pos > 0:
                    sent(rows.at[0, pl.ds(0, batches * (slots - reach - pos))], xs.at[1])


def shards(tokens, router_scores, expert_ids, gate_weight, up_weight, down_weight):
    blk_count = lax.axis_size("blk")
    rep_count = lax.axis_size("rep")
    count, depth = tokens.shape
    units = gate_weight.shape[1]
    window = blk_count * rep_count * units // FF
    gs = blk_count // window
    side = math.isqrt(blk_count)
    per_row = side // gs

    batches = len(BATCHES)
    slots = 2 * gs
    unit = side // 2
    many = slots * unit
    vmem = pl.BlockSpec(memory_space=pltpu.VMEM)
    hbm = pl.BlockSpec(memory_space=pltpu.HBM)
    dma = pltpu.SemaphoreType.DMA
    pieces = pltpu.VMEM((CAP * side, per_row, depth), BF16)
    blocks = pltpu.VMEM((batches * slots, unit, depth), BF16)
    parts = (batches, slots, unit, depth)
    single = pltpu.VMEM((batches, unit, depth), BF16)
    large = [
        pltpu.with_memory_space_constraint(a, pltpu.HBM)
        for a in (router_scores.T, expert_ids.T, tokens, gate_weight, up_weight, down_weight)
    ]
    return pl.pallas_call(
        functools.partial(moe_kernel, side, gs),
        out_shape=jax.ShapeDtypeStruct((count, depth), BF16),
        in_specs=[hbm] * len(large),
        out_specs=vmem,
        scratch_shapes=[
            pltpu.VMEM(router_scores.shape[::-1], F32),
            pltpu.VMEM(expert_ids.shape[::-1], jnp.int32),
            pltpu.VMEM((count, depth), BF16),
            pltpu.VMEM(gate_weight.shape, BF16),
            pltpu.VMEM(up_weight.shape, BF16),
            pltpu.VMEM(down_weight.shape, BF16),
            pltpu.VMEM((batches, count, side * per_row), BF16),
            pieces,
            pieces,
            pltpu.VMEM((2, batches * slots, unit, depth), BF16),
            single,
            pltpu.VMEM((2 * many, units), BF16),
            pltpu.VMEM(parts, F32),
            pltpu.VMEM(parts, BF16),
            pltpu.VMEM(parts, BF16),
            blocks,
            pltpu.VMEM((2, batches * slots, unit, depth), BF16),
            single,
            pieces,
            pieces,
            pltpu.VMEM((count, depth), F32),
            dma((6,)),
            dma((1,)),
            dma((batches,)),
            dma((2,)),
            dma((batches * slots,)),
            dma((1,)),
            dma((1,)),
            dma((batches,)),
            dma((1,)),
            dma((batches,)),
            dma((1,)),
            dma((batches * slots,)),
            dma((2, batches)),
            dma((batches,)),
            dma((1,)),
            dma((batches,)),
        ],
        compiler_params=pltpu.CompilerParams(
            collective_id=0, has_side_effects=True, vmem_limit_bytes=44 * 1024 * 1024
        ),
    )(*large)


def solution(mesh):
    placed = (
        P(("groups", "blk", "rep"), None),
        P(("groups", "blk", "rep"), None),
        P(("groups", "blk", "rep"), None),
        P(None, ("blk", "rep")),
        P(None, ("blk", "rep")),
        P(("blk", "rep"), None),
    )
    return jax.shard_map(
        shards,
        mesh=mesh,
        in_specs=placed,
        out_specs=P(("groups", "blk", "rep"), None),
        check_vma=False,
    )
```

```python
import functools
import math

import jax
import jax.numpy as jnp
from jax import lax
from jax.experimental import pallas as pl
from jax.experimental.pallas import tpu as pltpu
from jax.sharding import PartitionSpec as P

FF = 2048
CAP = 2
CHUNKS = 4

BATCHES = ((0, 0), (0, 1), (1, 1), (1, 0))
KINDS = "OFLGDBVRCUE"
ORDER = (
    0, 10, 201, 101, 20, 202, 102, 211, 30, 103, 111, 112, 203, 113, 121, 204, 212, 131,
    122, 205, 213, 300, 900, 400, 214, 1000, 221, 215, 132, 605, 231, 222, 310, 910, 410, 1010,
    123, 223, 232, 604, 615, 133, 224, 233, 603, 503, 614, 225, 234, 613, 602, 320, 502, 513,
    920, 235, 612, 420, 601, 1020, 330, 930, 625, 430, 1030, 624, 501, 623, 512, 523, 635, 634,
    622, 511, 633, 522, 533, 700, 611, 521, 632, 532, 621, 710, 531, 631, 720, 730, 800, 810,
    820, 830,
)

route_scale = 2.5

MESH = pl.DeviceIdType.MESH
BF16 = jnp.bfloat16
F32 = jnp.float32


def moe_kernel(
    side,
    gs,
    scores_hbm,
    ids_hbm,
    tok_hbm,
    wg_hbm,
    wu_hbm,
    wd_hbm,
    out_ref,
    scores_ref,
    ids_ref,
    tok,
    wg,
    wu,
    wd,
    mixes,
    send_y,
    recv_y,
    rows,
    oth,
    gate_acc,
    hidden,
    own_part,
    give,
    take,
    stage,
    came,
    oth_sum,
    send_r,
    recv_r,
    out_acc,
    load_sem,
    ys,
    yr,
    xs,
    xr,
    os_,
    ps,
    pr,
    qs,
    qr,
    rs,
    rf,
    rroot,
    tor,
    zs,
    zr,
):
    batches, unit, depth = oth.shape
    count, top = tok.shape[0], ids_ref.shape[0]
    width = depth // CHUNKS
    per_row = side // gs
    half = side // 2
    reach = gs // 2
    slots = gs + 2 * reach
    last = gs - 1
    most = last + reach
    blk = lax.axis_index("blk")
    rep = lax.axis_index("rep")
    y = lax.div(blk, side)
    x = lax.rem(blk, side)
    w = lax.rem(x, gs)
    me = w + reach
    my_half, my_m = lax.rem(y, 2), lax.div(y, 2)

    def at(yy, xx):
        return {"blk": yy * side + lax.rem(xx + side, side), "rep": rep}

    sign = jnp.where(w < reach, 1, -1)
    inner = jnp.logical_and(w > 0, w < last)
    up_side = jnp.where(w < reach, 0, 1)
    depth_in = jnp.minimum(w, last - w)
    up = at(y, x + sign)
    down = at(y, x - sign)
    partner = {"rep": 1 - rep}

    def row_of(rel, m):
        return m * 2 + lax.rem(my_half + rel, 2)

    def remote(src, dst, send, recv, dev):
        return pltpu.make_async_remote_copy(
            src_ref=src, dst_ref=dst, send_sem=send, recv_sem=recv, device_id=dev, device_id_type=MESH
        )

    def arrived(ref, recv):
        remote(ref, ref, recv, recv, partner).wait_recv()

    def sent(ref, send):
        remote(ref, ref, send, send, partner).wait_send()

    def per_cols(body):
        def step(c, _):
            body(pl.ds(pl.multiple_of(c * width, 128), width))
            return 0

        lax.fori_loop(0, CHUNKS, step, 0)

    load_tok = pltpu.make_async_copy(tok_hbm, tok, load_sem.at[0])
    loads = [
        pltpu.make_async_copy(src, dst, load_sem.at[k + 1])
        for k, (src, dst) in enumerate(((wg_hbm, wg), (wu_hbm, wu), (wd_hbm, wd)))
    ]
    tables = [
        pltpu.make_async_copy(src, dst, load_sem.at[4 + k])
        for k, (src, dst) in enumerate(((scores_hbm, scores_ref), (ids_hbm, ids_ref)))
    ]
    for load in tables:
        load.start()
    load_tok.start()

    barrier = pltpu.get_barrier_semaphore()
    for d in range(1, side):
        pl.semaphore_signal(barrier, inc=1, device_id=at(lax.rem(y + d, side), x), device_id_type=MESH)
    for hop in range(1, reach + 1):
        for dev in (at(y, x + hop), at(y, x - hop)):
            pl.semaphore_signal(barrier, inc=1, device_id=dev, device_id_type=MESH)
    pl.semaphore_signal(barrier, inc=1, device_id=partner, device_id_type=MESH)

    for load in tables:
        load.wait()
    spots = side * per_row
    sigmoid = 1.0 / (1.0 + jnp.exp(-scores_ref[...]))
    gates = route_scale * sigmoid / jnp.sum(sigmoid, axis=0, keepdims=True)
    spot = lax.broadcasted_iota(jnp.int32, (spots, count), 0)
    of_half = lax.rem(lax.div(spot, half * per_row) + my_half, 2)
    of_row = lax.rem(lax.div(spot, per_row), half) * 2 + of_half
    of_expert = of_row * per_row + lax.rem(lax.rem(spot, per_row) + lax.div(x, gs), per_row)
    ids = ids_ref[...]
    weight = jnp.zeros((spots, count), F32)
    hit = jnp.zeros((spots, count), F32)
    for k in range(top):
        same = ids[k : k + 1] == of_expert
        weight += jnp.where(same, gates[k : k + 1], 0.0)
        hit += jnp.where(same, 1.0, 0.0)
    before = lax.broadcasted_iota(jnp.int32, (count, count), 0) < lax.broadcasted_iota(
        jnp.int32, (count, count), 1
    )
    rank = jnp.dot(hit.astype(BF16), jnp.where(before, 1.0, 0.0).astype(BF16), preferred_element_type=F32)
    placed = [jnp.where(rank == s, hit, 0.0) for s in range(CAP)]

    load_tok.wait()
    for load in loads:
        load.start()

    def pack_rank(s):
        choose = placed[s].astype(BF16)

        def pack(cols):
            packed = jnp.dot(choose, tok[:, cols], preferred_element_type=F32)
            for p in range(side):
                send_y[s * side + p, :, cols] = packed[p * per_row : (p + 1) * per_row].astype(BF16)

        per_cols(pack)

    pack_rank(0)
    pl.semaphore_wait(barrier, side + 2 * reach)

    def exchange(b, source, first, into, send, recv):
        rel = BATCHES[b][1]
        dst = into.at[b * half + my_m]
        near = lambda d: -min(2 * d + rel, side - 2 * d - rel)
        for d in sorted(range(1 - rel, half), key=near):
            m = lax.rem(my_m + d + rel * my_half, half)
            remote(source.at[first + m], dst, send.at[0], recv.at[b], at(row_of(rel, m), x)).start()
        if rel == 0:
            pltpu.make_async_copy(source.at[first + my_m], dst, recv.at[b]).start()

    def forward(b, k, to_up, to_down):
        at_k = b * slots + k
        ref = rows.at[0, at_k]
        if to_up:
            remote(ref, ref, xs.at[0], xr.at[at_k], up).start()

        if to_down:

            @pl.when(inner)
            def _():
                remote(ref, ref, xs.at[1], xr.at[at_k], down).start()

        remote(ref, rows.at[1, at_k], ps.at[0], pr.at[b], partner).start()

    def y_task(b, _):
        s, rel = BATCHES[b]
        exchange(b, send_y, s * side + rel * half, recv_y, ys, yr)

    def own_task(b, _):
        arrived(recv_y.at[pl.ds(b * half, half)], yr.at[b])

        def body(cols):
            parts = [recv_y[b * half + m, :, cols].astype(F32) for m in range(half)]
            oth[b, :, cols] = jnp.concatenate([p[1:2] for p in parts], axis=0).astype(BF16)
            rows[0, b * slots + me, :, cols] = jnp.concatenate([p[:1] for p in parts], axis=0).astype(BF16)

        per_cols(body)
        near = w < reach
        hop = jnp.where(near, -(w + 1), gs - w)
        slot = b * slots + jnp.where(near, reach + gs + w, w - gs + reach)
        remote(oth.at[b], rows.at[0, slot], os_.at[0], xr.at[slot], at(y, x + hop)).start()
        forward(b, me, True, True)

    def when_far(i, most_in, body):
        if i > most_in:
            pl.when(inner)(body)
        else:
            body()

    def forward_up_task(b, i):
        def body():
            k = me - sign * i
            arrived(rows.at[0, b * slots + k], xr.at[b * slots + k])
            forward(b, k, True, False)

        when_far(i, reach, body)

    def forward_down_task(b, i):
        def body():
            k = me + sign * i
            arrived(rows.at[0, b * slots + k], xr.at[b * slots + k])
            forward(b, k, False, True)

        if i == most:
            pl.when(jnp.logical_not(inner))(body)
        else:
            body()

    many = slots * unit

    loaded = []

    def gate_task(b, _):
        if not loaded:
            loaded.append(b)
            for load in loads:
                load.wait()
        arrived(rows.at[1, pl.ds(b * slots, slots)], pr.at[b])
        block = rows[:, b * slots : (b + 1) * slots].reshape(2 * many, depth)
        gate_acc[...] = jnp.dot(block, wg[...], preferred_element_type=F32)

    def up_task(b, _):
        block = rows[:, b * slots : (b + 1) * slots].reshape(2 * many, depth)
        gate = gate_acc[...]
        up = jnp.dot(block, wu[...], preferred_element_type=F32)
        hidden[...] = (gate / (1.0 + jnp.exp(-gate)) * up).astype(BF16)

    def down_task(part_at, b, _):
        def step(c, _):
            cols = pl.ds(pl.multiple_of(c * width, 128), width)
            part = jnp.dot(hidden[...], wd[:, cols], preferred_element_type=F32)
            give[b, :, :, cols] = part[many:].astype(BF16).reshape(slots, unit, width)
            own_part[b, :, :, cols] = part[:many].reshape(slots, unit, width)
            ours, theirs = give.at[b, :, :, cols], take.at[b, :, :, cols]
            remote(ours, theirs, qs.at[0], qr.at[b], partner).start()
            return 0

        lax.fori_loop(part_at * CHUNKS // 2, (part_at + 1) * CHUNKS // 2, step, 0)

    took = []

    def partial_sum(b, k, side_in, at_in):
        at_k = b * slots + k

        def body(cols):
            total = own_part[b, k, :, cols] + take[b, k, :, cols].astype(F32)
            if at_in:
                total += came.at[side_in][at_k, :, cols].astype(F32)
            stage[at_k, :, cols] = total.astype(BF16)

        if at_in:
            arrived(came.at[side_in, at_k], rf.at[at_k])
        per_cols(body)

    def taken(b):
        if b not in took:
            took.append(b)
            arrived(take.at[b], qr.at[b])

    def back_down_task(b, i):
        taken(b)

        def body():
            k = me - sign * i
            at_k = b * slots + k
            partial_sum(b, k, up_side, True)
            src = stage.at[at_k]
            recv = rroot.at[up_side, b] if i == 1 else rf.at[at_k]

            @pl.when(inner)
            def _():
                remote(src, came.at[up_side, at_k], rs.at[0], recv, down).start()

            @pl.when(jnp.logical_not(inner))
            def _():
                remote(src, oth_sum.at[b], rs.at[0], tor.at[b], at(y, x - sign * i)).start()

        when_far(i, reach, body)

    def back_up_task(b, i):
        taken(b)
        k = me + sign * i
        at_k = b * slots + k
        recv = rroot.at[1 - up_side, b] if i == 1 else rf.at[at_k]

        @pl.when(jnp.logical_not(inner))
        def _():
            partial_sum(b, k, 1 - up_side, False)

        if i < most:

            @pl.when(inner)
            def _():
                partial_sum(b, k, 1 - up_side, True)

        def body():
            remote(stage.at[at_k], came.at[1 - up_side, at_k], rs.at[0], recv, up).start()

        if i == most:
            pl.when(jnp.logical_not(inner))(body)
        else:
            body()

    def root_task(b, _):
        at_me = b * slots + me

        def body(cols):
            own_part[b, me, :, cols] += take[b, me, :, cols].astype(F32)

        per_cols(body)

        def add(side_in):
            arrived(came.at[side_in, at_me], rroot.at[side_in, b])

            def body(cols):
                own_part[b, me, :, cols] += came.at[side_in][at_me, :, cols].astype(F32)

            per_cols(body)

        add(up_side)
        pl.when(inner)(lambda: add(1 - up_side))
        arrived(oth_sum.at[b], tor.at[b])

        def split(cols):
            total = own_part[b, me, :, cols]
            other = oth_sum[b, :, cols].astype(F32)
            for m in range(half):
                pair = jnp.concatenate([total[m : m + 1], other[m : m + 1]], axis=0)
                send_r[b * half + m, :, cols] = pair.astype(BF16)

        per_cols(split)
        exchange(b, send_r, b * half, recv_r, zs, zr)

    combined = []

    def combine_task(b, _):
        arrived(recv_r.at[pl.ds(b * half, half)], zr.at[b])
        mix = mixes[b]
        begin, end = not combined, len(combined) == batches - 1
        combined.append(b)

        def body(cols):
            parts = [recv_r[b * half + m, :, cols].astype(F32) for m in range(half)]
            block = jnp.concatenate(parts + parts, axis=0).astype(BF16)
            total = jnp.dot(mix, block, preferred_element_type=F32)
            if not begin:
                total += out_acc[:, cols]
            if end:
                out_ref[:, cols] = total.astype(BF16)
            else:
                out_acc[:, cols] = total

        per_cols(body)

    tasks = (
        own_task,
        forward_up_task,
        forward_down_task,
        gate_task,
        functools.partial(down_task, 0),
        back_down_task,
        back_up_task,
        root_task,
        combine_task,
        up_task,
        functools.partial(down_task, 1),
    )
    for s in range(CAP):
        if s > 0:
            pack_rank(s)
        for b in range(batches):
            if BATCHES[b][0] == s:
                y_task(b, 0)

    n = half * per_row
    eye = (
        lax.broadcasted_iota(jnp.int32, (n, n), 0) == lax.broadcasted_iota(jnp.int32, (n, n), 1)
    ).astype(F32).astype(BF16)
    for b, (s, rel) in enumerate(BATCHES):
        mix = (placed[s] * weight)[rel * n : (rel + 1) * n]
        mix_hi = mix.astype(BF16)
        mix_lo = (mix - mix_hi.astype(F32)).astype(BF16)
        turned = [
            lax.dot_general(m, eye, (((0,), (0,)), ((), ())), preferred_element_type=F32)
            for m in (mix_hi, mix_lo)
        ]
        mixes[b] = jnp.concatenate(turned, axis=1).astype(BF16)

    for code in ORDER:
        kind, b, i = code // 100, code // 10 % 10, code % 10
        with jax.named_scope(f"{KINDS[kind]}{b}{i}"):
            tasks[kind](b, i)

    with jax.named_scope("drain"):
        away = CAP * (side - 1)
        sent(send_y.at[pl.ds(0, away)], ys.at[0])
        sent(send_r.at[pl.ds(0, away)], zs.at[0])
        sent(oth, os_.at[0])
        sent(rows.at[0], ps.at[0])
        sent(give, qs.at[0])
        sent(stage.at[pl.ds(0, batches * (slots - 1))], rs.at[0])
        for pos in range(reach):

            @pl.when(depth_in == pos)
            def _():
                sent(rows.at[0, pl.ds(0, batches * (pos + reach + 1))], xs.at[0])
                if pos > 0:
                    sent(rows.at[0, pl.ds(0, batches * (slots - reach - pos))], xs.at[1])


def shards(tokens, router_scores, expert_ids, gate_weight, up_weight, down_weight):
    blk_count = lax.axis_size("blk")
    rep_count = lax.axis_size("rep")
    count, depth = tokens.shape
    units = gate_weight.shape[1]
    window = blk_count * rep_count * units // FF
    gs = blk_count // window
    side = math.isqrt(blk_count)
    per_row = side // gs

    batches = len(BATCHES)
    slots = 2 * gs
    unit = side // 2
    many = slots * unit
    vmem = pl.BlockSpec(memory_space=pltpu.VMEM)
    hbm = pl.BlockSpec(memory_space=pltpu.HBM)
    dma = pltpu.SemaphoreType.DMA
    pieces = pltpu.VMEM((CAP * side, per_row, depth), BF16)
    blocks = pltpu.VMEM((batches * slots, unit, depth), BF16)
    parts = (batches, slots, unit, depth)
    single = pltpu.VMEM((batches, unit, depth), BF16)
    large = [
        pltpu.with_memory_space_constraint(a, pltpu.HBM)
        for a in (router_scores.T, expert_ids.T, tokens, gate_weight, up_weight, down_weight)
    ]
    return pl.pallas_call(
        functools.partial(moe_kernel, side, gs),
        out_shape=jax.ShapeDtypeStruct((count, depth), BF16),
        in_specs=[hbm] * len(large),
        out_specs=vmem,
        scratch_shapes=[
            pltpu.VMEM(router_scores.shape[::-1], F32),
            pltpu.VMEM(expert_ids.shape[::-1], jnp.int32),
            pltpu.VMEM((count, depth), BF16),
            pltpu.VMEM(gate_weight.shape, BF16),
            pltpu.VMEM(up_weight.shape, BF16),
            pltpu.VMEM(down_weight.shape, BF16),
            pltpu.VMEM((batches, count, side * per_row), BF16),
            pieces,
            pieces,
            pltpu.VMEM((2, batches * slots, unit, depth), BF16),
            single,
            pltpu.VMEM((2 * many, units), F32),
            pltpu.VMEM((2 * many, units), BF16),
            pltpu.VMEM(parts, F32),
            pltpu.VMEM(parts, BF16),
            pltpu.VMEM(parts, BF16),
            blocks,
            pltpu.VMEM((2, batches * slots, unit, depth), BF16),
            single,
            pieces,
            pieces,
            pltpu.VMEM((count, depth), F32),
            dma((6,)),
            dma((1,)),
            dma((batches,)),
            dma((2,)),
            dma((batches * slots,)),
            dma((1,)),
            dma((1,)),
            dma((batches,)),
            dma((1,)),
            dma((batches,)),
            dma((1,)),
            dma((batches * slots,)),
            dma((2, batches)),
            dma((batches,)),
            dma((1,)),
            dma((batches,)),
        ],
        compiler_params=pltpu.CompilerParams(
            collective_id=0, has_side_effects=True, vmem_limit_bytes=44 * 1024 * 1024
        ),
    )(*large)


def solution(mesh):
    placed = (
        P(("groups", "blk", "rep"), None),
        P(("groups", "blk", "rep"), None),
        P(("groups", "blk", "rep"), None),
        P(None, ("blk", "rep")),
        P(None, ("blk", "rep")),
        P(("blk", "rep"), None),
    )
    return jax.shard_map(
        shards,
        mesh=mesh,
        in_specs=placed,
        out_specs=P(("groups", "blk", "rep"), None),
        check_vma=False,
    )
```
